32 devices in a mesh: grp: 4 (over y, x), dom: 8 (over z, core).
Axes of the slice: x: 2, y: 2, z: 4, core: 2. Of those that a mesh axis runs over, the one named last changes fastest.
Arguments:
- fields: float32 [210, 32768], P(None, ('grp', 'dom')), may hold values from -6 to 6
- metric: float32 [9, 32768], P(None, ('grp', 'dom')), may hold values from -5 to 5
- normals: float32 [12, 32768], P(None, ('grp', 'dom')), may hold values from -3 to 3
- fscale: float32 [4, 32768], P(None, ('grp', 'dom')), may hold values from 0.5 to 4
- orders: int32 [32768], P(('grp', 'dom')), may hold values from 1 to 4, as said below
- slots: int32 [32768], P(('grp', 'dom')), may hold values from 0 to 511, as said below
- send_faces: int32 [294912], P(('grp', 'dom')), may hold values from 0 to 8192, as said below
- recv_faces: int32 [262144], P(('grp', 'dom')), may hold values from 0 to 9216, as said below
- dmat: float32 [4, 105, 35], P('grp'), may hold values from -4 to 4
- tmat: float32 [4, 60, 35], P('grp'), may hold values from -4 to 4
- lmat: float32 [4, 35, 60], P('grp'), may hold values from -3 to 3
Outputs:
- rhs: float32 [210, 65536], P(None, ('grp', 'dom'))
The draws below stay inside these ranges and needn't reach their ends.
Inputs may be any that keep to these rules, and one draw needn't show every extreme that they name: `orders`: on each device every order from 1 to 4 is held by at least one element and by at most 512; one order is held by exactly 512. The elements of one device that share an order have distinct slots. `send_faces`: each entry names a face of an occupied slot of the sending bucket or equals 4 * 2048 (nothing); in each list the items in use stand first. `recv_faces`: every face of an occupied slot names a distinct received item that is in use, and every item in use is named by exactly one face; faces of empty slots hold 9216. A list carries at most 768 items in use, and some list carries exactly 768.
All inputs are finite; a program needn't handle non-finite values.
Results may differ from the reference program's by a relative error of at most 0.0003.
Values sent between devices are 32-bit elements; how exact they have to be, the bound alone decides.
A program may use at most 128 MiB of HBM per device.

```python
import math
import jax
import jax.numpy as jnp
from jax import lax

NPM = 35
FPTS = 15
ORDERS = 4
E_DEV = 1024
CAP = 512
NB = 2048
FCAP = 768
LISTS = 9216
DOMS = 8
ELEMS = 32768
SLOTS = 65536
DEVICES = 32


def mesh_tables(key):
    base = jax.random.fold_in(key, 4242)
    streams = jax.random.split(base, 7)
    spare = E_DEV - CAP
    leading = jax.random.randint(streams[0], (DEVICES,), 0, ORDERS)
    cuts = jax.random.randint(streams[1], (DEVICES, 2), 0, spare - 2)
    lower = jnp.minimum(cuts[:, 0], cuts[:, 1]) + 1
    upper = jnp.maximum(cuts[:, 0], cuts[:, 1]) + 2
    rank_sizes = jnp.stack([jnp.full((DEVICES,), CAP, jnp.int32), lower, upper - lower, spare - upper], 1)
    rank_ends = jnp.cumsum(rank_sizes, 1)
    rank_starts = rank_ends - rank_sizes
    position = jax.vmap(lambda sub_key: jax.random.permutation(sub_key, E_DEV))(jax.random.split(streams[2], DEVICES)).astype(jnp.int32)
    rank_of = jnp.sum((position[:, :, None] >= rank_ends[:, None, :]).astype(jnp.int32), 2)
    within = position - jnp.take_along_axis(rank_starts, rank_of, 1)
    order_index = (leading[:, None] + rank_of) % ORDERS
    shuffles = jax.vmap(lambda sub_key: jax.random.permutation(sub_key, CAP))(jax.random.split(streams[3], DEVICES * ORDERS)).astype(jnp.int32)
    shuffles = shuffles.reshape(DEVICES, ORDERS * CAP)
    slot_value = jnp.take_along_axis(shuffles, order_index * CAP + within, 1)
    device_ids = jnp.arange(DEVICES, dtype=jnp.int32)[:, None]
    bucket_dev = order_index * DOMS + device_ids % DOMS
    bucket_col = device_ids // DOMS * CAP + slot_value
    occupied = jnp.zeros((DEVICES, NB), jnp.int32).at[bucket_dev, bucket_col].set(1)
    face_total = 4 * jnp.sum(occupied, 1)
    occupied_slots = jnp.argsort((1 - occupied) * NB + jnp.arange(NB, dtype=jnp.int32)[None], axis=1).astype(jnp.int32)
    enumerated = jnp.arange(4 * NB, dtype=jnp.int32)
    face_of = (enumerated % 4)[None] * NB + occupied_slots[:, enumerated // 4]
    valid = enumerated[None] < face_total[:, None]
    list_total = 3 * ORDERS
    first_list = jax.random.randint(streams[4], (DEVICES,), 0, list_total)
    leading_count = jnp.minimum(face_total, FCAP)
    remainder = face_total - leading_count
    share = remainder // (list_total - 1)
    extra = remainder % (list_total - 1)
    offset = (jnp.arange(list_total, dtype=jnp.int32)[None] - first_list[:, None]) % list_total
    counts = jnp.where(offset == 0, leading_count[:, None], share[:, None] + (offset - 1 < extra[:, None]).astype(jnp.int32))
    list_ends = jnp.cumsum(counts, 1)
    list_starts = list_ends - counts
    face_shuffle = jax.vmap(lambda sub_key: jax.random.permutation(sub_key, 4 * NB))(jax.random.split(streams[5], DEVICES)).astype(jnp.int32)
    scores = jnp.where(valid, face_shuffle, 4 * NB + enumerated[None])
    ranking = jnp.argsort(jnp.argsort(scores, axis=1), axis=1).astype(jnp.int32)
    list_of = jnp.sum((ranking[:, :, None] >= list_ends[:, None, :]).astype(jnp.int32), 2)
    list_of = jnp.minimum(list_of, list_total - 1)
    place_in = ranking - jnp.take_along_axis(list_starts, list_of, 1)
    entry_value = jnp.where(valid, list_of * FCAP + place_in, LISTS)
    targets = jnp.where(valid, face_of, 4 * NB)
    receive = jnp.full((DEVICES, 4 * NB + 1), LISTS, jnp.int32).at[device_ids, targets].set(entry_value)[:, :4 * NB]
    sender_ids = jnp.arange(DEVICES, dtype=jnp.int32)[:, None, None]
    direction = jnp.arange(3, dtype=jnp.int32)[None, :, None]
    peer_group = jnp.arange(ORDERS, dtype=jnp.int32)[None, None, :]
    receiver = peer_group * DOMS + (sender_ids % DOMS + direction - 1) % DOMS
    list_index = direction * ORDERS + sender_ids // DOMS
    wanted = counts[receiver, list_index]
    picks = jax.random.randint(streams[6], (DEVICES, 3, ORDERS, FCAP), 0, 2 ** 30) % face_total[:, None, None, None]
    chosen = jnp.take_along_axis(face_of, picks.reshape(DEVICES, -1), 1).reshape(DEVICES, 3, ORDERS, FCAP)
    sending = jnp.where(jnp.arange(FCAP, dtype=jnp.int32)[None, None, None] < wanted[..., None], chosen, 4 * NB)
    return ((order_index + 1).reshape(ELEMS), slot_value.reshape(ELEMS), sending.reshape(DEVICES * LISTS), receive.reshape(DEVICES * 4 * NB))


def draw_orders(key, part):
    return mesh_tables(key)[0]


def draw_slots(key, part):
    return mesh_tables(key)[1]


def draw_send_faces(key, part):
    return mesh_tables(key)[2]


def draw_recv_faces(key, part):
    return mesh_tables(key)[3]


def block_levels(rng, extent, shards, least, largest):
    factor_of = 1.0
    for dim, shards_of in shards:
        draws = jax.random.uniform(jax.random.fold_in(jax.random.fold_in(rng, 6), dim), (shards_of,), jnp.float32, least / len(shards), largest / len(shards))
        factor_of = factor_of * jnp.repeat(jnp.exp(draws), extent[dim] // shards_of).reshape((-1,) + (1,) * (len(extent) - 1 - dim))
    return factor_of


def bell_draw(rng, shape, deviation, bound, cuts=(), kind=jnp.bfloat16):
    level = block_levels(rng, shape, cuts, -0.22, 0.18) if cuts else 1.0
    values = jax.random.normal(rng, shape, jnp.float32) * deviation * level
    return jnp.minimum(jnp.maximum(values, -bound), bound).astype(kind)


def setup_inputs(seed: int = 0) -> dict:
    key_list = jax.random.split(jax.random.key(seed), 12)
    return {
        "fields": bell_draw(key_list[0], (6 * NPM, ELEMS), 1.0, 6.0, ((1, 32),), jnp.float32),
        "metric": bell_draw(key_list[1], (9, ELEMS), 1.0, 5.0, ((1, 32),), jnp.float32),
        "normals": bell_draw(key_list[2], (12, ELEMS), 0.6, 3.0, ((1, 32),), jnp.float32),
        "fscale": jnp.clip(jnp.exp(math.log(4.0) - 2.0794415 * jax.random.uniform(key_list[3], (4, ELEMS), jnp.float32) ** block_levels(key_list[3], (4, ELEMS), ((1, 32),), -0.2, 0.2)), 0.5, 4.0),
        "orders": draw_orders(jax.random.fold_in(key_list[11], 71), 0),
        "slots": draw_slots(jax.random.fold_in(key_list[11], 71), 0),
        "send_faces": draw_send_faces(jax.random.fold_in(key_list[11], 71), 0),
        "recv_faces": draw_recv_faces(jax.random.fold_in(key_list[11], 71), 0),
        "dmat": bell_draw(key_list[8], (ORDERS, 3 * NPM, NPM), 0.3, 4.0, ((0, 4),), jnp.float32),
        "tmat": bell_draw(key_list[9], (ORDERS, 4 * FPTS, NPM), 0.3, 4.0, ((0, 4),), jnp.float32),
        "lmat": bell_draw(key_list[10], (ORDERS, NPM, 4 * FPTS), 0.2, 3.0, ((0, 4),), jnp.float32),
    }


exact_prec = lax.Precision.HIGHEST


def order_mask(order_index):
    node_total = (order_index + 2) * (order_index + 3) * (order_index + 4) // 6
    return (jnp.arange(NPM, dtype=jnp.int32) < node_total).astype(jnp.float32)


def cross_of(first_vec, second_vec):
    return [first_vec[1] * second_vec[2] - first_vec[2] * second_vec[1],
            first_vec[2] * second_vec[0] - first_vec[0] * second_vec[2],
            first_vec[0] * second_vec[1] - first_vec[1] * second_vec[0]]


def volume_terms(coefficients, metric_cols, deriv_mats):
    derived = jnp.einsum('anm,qms->qans', deriv_mats, coefficients, precision=exact_prec)

    def partial_of(component, direction):
        return (metric_cols[0, direction][None] * derived[component, 0]
                + metric_cols[1, direction][None] * derived[component, 1]
                + metric_cols[2, direction][None] * derived[component, 2])

    curl_h = [partial_of(5, 1) - partial_of(4, 2), partial_of(3, 2) - partial_of(5, 0), partial_of(4, 0) - partial_of(3, 1)]
    curl_e = [partial_of(2, 1) - partial_of(1, 2), partial_of(0, 2) - partial_of(2, 0), partial_of(1, 0) - partial_of(0, 1)]
    return jnp.stack(curl_h + [-value for value in curl_e], 0)


def face_flux(own_traces, neighbour, normal_cols, scale_cols):
    own_split = own_traces.reshape(6, FPTS, -1)
    far_split = neighbour.reshape(6, FPTS, -1)
    jump_e = [far_split[c] - own_split[c] for c in range(3)]
    jump_h = [far_split[c + 3] - own_split[c + 3] for c in range(3)]
    normal = [normal_cols[c] for c in range(3)]
    normal_e = normal[0] * jump_e[0] + normal[1] * jump_e[1] + normal[2] * jump_e[2]
    normal_h = normal[0] * jump_h[0] + normal[1] * jump_h[1] + normal[2] * jump_h[2]
    turn_h = cross_of(normal, jump_h)
    turn_e = cross_of(normal, jump_e)
    flux_e = [0.5 * scale_cols * (turn_h[c] + jump_e[c] - normal[c] * normal_e) for c in range(3)]
    flux_h = [0.5 * scale_cols * (-turn_e[c] + jump_h[c] - normal[c] * normal_h) for c in range(3)]
    return jnp.stack(flux_e + flux_h, 0)


def block_rhs(bucket, own_traces, neighbour, deriv_mats, lift_mat):
    slot_count = bucket.shape[1]
    coefficients = bucket[:6 * NPM].reshape(6, NPM, slot_count)
    metric_cols = bucket[6 * NPM:6 * NPM + 9].reshape(3, 3, slot_count)
    normal_cols = bucket[6 * NPM + 9:6 * NPM + 21].reshape(3, 1, 4 * slot_count)
    scale_cols = bucket[6 * NPM + 21:6 * NPM + 25].reshape(1, 4 * slot_count)
    volume = volume_terms(coefficients, metric_cols, deriv_mats)
    flux = face_flux(own_traces, neighbour, normal_cols, scale_cols).reshape(6, FPTS * 4, slot_count)
    lifted = jnp.einsum('mp,qps->qms', lift_mat, flux, precision=exact_prec)
    return (volume + lifted).reshape(6 * NPM, slot_count)


def reference(fields, metric, normals, fscale, orders, slots, send_faces, recv_faces, dmat, tmat, lmat):
    element_total = fields.shape[1]
    positions = jnp.arange(element_total, dtype=jnp.int32)
    owner = positions // E_DEV
    column = ((orders - 1) * DOMS + owner % DOMS) * NB + (owner // DOMS) * CAP + slots
    inverse = jnp.full((SLOTS,), element_total, jnp.int32).at[column].set(positions)
    payload = jnp.concatenate([fields, metric, normals, fscale], 0)
    padded = jnp.concatenate([payload, jnp.zeros((payload.shape[0], 1), jnp.float32)], 1)

    def gather_block(block_id):
        picked = lax.dynamic_slice_in_dim(inverse, block_id * NB, NB)
        return jnp.take(padded, picked, axis=1)

    def matrices(block_id):
        order_index = block_id // DOMS
        node_mask = order_mask(order_index)
        deriv_mats = dmat[order_index].reshape(3, NPM, NPM) * node_mask[None, :, None] * node_mask[None, None, :]
        trace_mat = tmat[order_index] * node_mask[None, :]
        lift_mat = lmat[order_index] * node_mask[:, None]
        return deriv_mats, trace_mat, lift_mat

    def traces_of(block_id):
        bucket = gather_block(block_id)
        trace_mat = matrices(block_id)[1]
        coefficients = bucket[:6 * NPM].reshape(6, NPM, NB)
        traced = jnp.einsum('pm,qms->qps', trace_mat, coefficients, precision=exact_prec)
        return traced.reshape(6 * FPTS, 4 * NB)

    traces = lax.map(traces_of, jnp.arange(DEVICES, dtype=jnp.int32))
    entries = jnp.arange(LISTS, dtype=jnp.int32)
    direction = entries // (ORDERS * FCAP)
    peer_group = (entries // FCAP) % ORDERS
    places = entries % FCAP
    receiver = jnp.arange(DEVICES, dtype=jnp.int32)[:, None]
    sender = peer_group[None] * DOMS + (receiver % DOMS - direction[None] + 1) % DOMS
    position = (direction[None] * ORDERS + receiver // DOMS) * FCAP + places[None]
    send_table = send_faces.reshape(DEVICES, LISTS)
    sent_face = send_table[sender, position]
    missing = DEVICES * 4 * NB
    flat_id = jnp.where(sent_face < 4 * NB, sender * (4 * NB) + sent_face, missing)
    recv_table = recv_faces.reshape(DEVICES, 4 * NB)

    def rhs_of(block_id):
        bucket = gather_block(block_id)
        deriv_mats, trace_mat, lift_mat = matrices(block_id)
        entry_ids = recv_table[block_id]
        global_ids = flat_id[block_id][jnp.minimum(entry_ids, LISTS - 1)]
        global_ids = jnp.where(entry_ids < LISTS, global_ids, missing)
        valid = (global_ids < missing).astype(jnp.float32)
        src_block = jnp.minimum(global_ids // (4 * NB), DEVICES - 1)
        face_ids = global_ids % (4 * NB)
        neighbour = traces[src_block, :, face_ids].T * valid[None]
        return block_rhs(bucket, traces[block_id], neighbour, deriv_mats, lift_mat)

    blocks = lax.map(rhs_of, jnp.arange(DEVICES, dtype=jnp.int32))
    return jnp.transpose(blocks, (1, 0, 2)).reshape(6 * NPM, SLOTS)
```

```python
import functools

import jax
import jax.numpy as jnp
from jax import lax
from jax.experimental import pallas as pl
from jax.experimental.pallas import tpu as pltpu
from jax.sharding import PartitionSpec as P

NPM = 35
FPTS = 15
COMPS = 6
FACES = 4
PP = 16
DP = 40
LANES = 128
TR = COMPS * PP
GEO = COMPS * NPM
METRIC, NORMAL, SCALE = GEO, GEO + 9, GEO + 21
ROWS = GEO + 30
BIG = 3 * DP + FACES * PP
MESH = pl.DeviceIdType.MESH
VMEM_LIMIT = 60 * 1024 * 1024


def split(x):
    high = x.astype(jnp.bfloat16)
    low = (x - high.astype(jnp.float32)).astype(jnp.bfloat16)
    return high, low


def dot3(a, b, dims):
    ah, al = a
    bh, bl = b

    def mul(x, y):
        return lax.dot_general(x, y, (dims, ((), ())), preferred_element_type=jnp.float32)

    return mul(ah, bh) + (mul(ah, bl) + mul(al, bh))


def params(**kw):
    return pltpu.CompilerParams(vmem_limit_bytes=VMEM_LIMIT, **kw)


VM = pl.BlockSpec(memory_space=pltpu.VMEM)
SM = pl.BlockSpec(memory_space=pltpu.SMEM)


def bucket_kernel(groups, cap, target_ref, fields_ref, metric_ref, normals_ref, fscale_ref, out_ref, pay):
    pay[0:GEO, :] = fields_ref[...]
    pay[METRIC : METRIC + 9, :] = metric_ref[...]
    pay[NORMAL : NORMAL + 12, :] = normals_ref[...]
    pay[SCALE : SCALE + 4, :] = fscale_ref[...]
    pay[SCALE + 4 : ROWS, :] = jnp.zeros((ROWS - SCALE - 4, pay.shape[1]), jnp.float32)
    high, low = split(pay[...])
    elements = pay.shape[1]
    target = target_ref[...]
    step = min(cap, 256)
    for g in range(groups):
        for k in range(0, cap, step):
            ids = lax.broadcasted_iota(jnp.int32, (step, elements), 0) + (g * cap + k)
            hot = jnp.where(ids == target, 1.0, 0.0).astype(jnp.bfloat16)
            dims = (((1,), (1,)), ((), ()))
            out_ref[g, :, k : k + step] = lax.dot_general(
                high, hot, dims, preferred_element_type=jnp.float32
            ) + lax.dot_general(low, hot, dims, preferred_element_type=jnp.float32)


def gather_block(index_ref, base, table, tmp):
    for i in range(LANES):
        tmp[i : i + 1, :] = table[pl.ds(index_ref[base + i], 1), :]


def send_kernel(groups, cap, lists, list_size, send_ref, bucket_ref, tt_ref, out_ref, table, tmp):
    slots = groups * cap
    weights = split(tt_ref[...])
    for g in range(groups):
        coefs = split(bucket_ref[g])
        for f in range(FACES):
            w = tuple(x[f * LANES : (f + 1) * LANES, :] for x in weights)
            table[f * slots + g * cap : f * slots + (g + 1) * cap, :] = dot3(coefs, w, ((0,), (1,)))
    table[FACES * slots : FACES * slots + 8, :] = jnp.zeros((8, LANES), jnp.float32)

    def one_list(item, _):
        for q in range(list_size // LANES):
            gather_block(send_ref, item * list_size + q * LANES, table, tmp.at[q % 2])
            out_ref[item, :, q * LANES : (q + 1) * LANES] = tmp[q % 2].T[:TR]
        return 0

    lax.fori_loop(0, lists, one_list, 0)


def exchange_kernel(groups, doms, lists_ref, out_ref, send_sem, recv_sem, local_sem):
    g = lax.axis_index("grp")
    p = lax.axis_index("dom")
    plan = [(d, j) for d in range(1, groups) for j in range(3)] + [(0, 0), (0, 2)]
    barrier = pltpu.get_barrier_semaphore()

    def peer(d, j):
        return (lax.rem(g + d, groups), lax.rem(p + j - 1 + doms, doms))

    for d, j in plan:
        pl.semaphore_signal(barrier, inc=1, device_id=peer(d, j), device_id_type=MESH)
    pl.semaphore_wait(barrier, len(plan))
    order = sorted(plan, key=lambda x: (x[0] != 2, x[0] == 0))
    copies = []
    for d, j in order:
        h = lax.rem(g + d, groups)
        copy = pltpu.make_async_remote_copy(
            src_ref=lists_ref.at[j * groups + h],
            dst_ref=out_ref.at[j * groups + g],
            send_sem=send_sem.at[d * 3 + j],
            recv_sem=recv_sem.at[d * 3 + j],
            device_id=peer(d, j),
            device_id_type=MESH,
        )
        copy.start()
        copies.append(copy)
    own = pltpu.make_async_copy(lists_ref.at[groups + g], out_ref.at[groups + g], local_sem)
    own.start()
    for d, j in order:
        src = lax.rem(g - d + groups, groups)
        pltpu.make_async_remote_copy(
            src_ref=lists_ref.at[j * groups + src],
            dst_ref=out_ref.at[j * groups + src],
            send_sem=send_sem.at[d * 3 + j],
            recv_sem=recv_sem.at[d * 3 + j],
            device_id=peer(d, j),
            device_id_type=MESH,
        ).wait_recv()
    for copy in copies:
        copy.wait_send()
    own.wait()


def cross_of(u, v):
    return [u[1] * v[2] - u[2] * v[1], u[2] * v[0] - u[0] * v[2], u[0] * v[1] - u[1] * v[0]]


CURL = ((5, 1, 4, 2), (3, 2, 5, 0), (4, 0, 3, 1), (1, 2, 2, 1), (2, 0, 0, 2), (0, 1, 1, 0))


def final_kernel(
    groups, cap, lists, list_size, recv_ref, arrived_ref, bucket_ref, tt_ref, big_ref, out_ref, table, tmp, far, flux, stack
):
    slots = groups * cap
    fill = jnp.zeros((LANES - TR, LANES), jnp.float32)

    def one_list(item, _):
        for q in range(list_size // LANES):
            block = jnp.concatenate([arrived_ref[item, :, q * LANES : (q + 1) * LANES], fill], 0)
            table[pl.ds(pl.multiple_of(item * list_size + q * LANES, LANES), LANES), :] = block.T
        return 0

    lax.fori_loop(0, lists, one_list, 0)
    table[lists * list_size : lists * list_size + 8, :] = jnp.zeros((8, LANES), jnp.float32)
    stack[...] = jnp.zeros_like(stack)
    weights = split(tt_ref[...])
    big = split(big_ref[...])

    for g in range(groups):

        def one_face(f, _):
            for q in range(cap // LANES):
                gather_block(recv_ref, f * slots + g * cap + q * LANES, table, tmp.at[q % 2])
                far[f, :, q * LANES : (q + 1) * LANES] = tmp[q % 2].T[:TR]
            return 0

        lax.fori_loop(0, FACES, one_face, 0)
        block = bucket_ref[g]
        pieces = split(block)
        for f in range(FACES):
            own = dot3(tuple(x[f * LANES : f * LANES + TR, :] for x in weights), pieces, ((1,), (0,)))
            jump = far[f] - own
            jumps = [jump[c * PP : (c + 1) * PP, :] for c in range(COMPS)]
            n = [block[NORMAL + c * FACES + f : NORMAL + c * FACES + f + 1, :] for c in range(3)]
            s = 0.5 * block[SCALE + f : SCALE + f + 1, :]
            je, jh = jumps[:3], jumps[3:]
            ne = n[0] * je[0] + n[1] * je[1] + n[2] * je[2]
            nh = n[0] * jh[0] + n[1] * jh[1] + n[2] * jh[2]
            th, te = cross_of(n, jh), cross_of(n, je)
            for c in range(3):
                flux[c, f * PP : (f + 1) * PP, :] = s * (th[c] + je[c] - n[c] * ne)
                flux[3 + c, f * PP : (f + 1) * PP, :] = s * (jh[c] - te[c] - n[c] * nh)
        coefs = [bucket_ref[g, c * NPM : (c + 1) * NPM, :] for c in range(COMPS)]
        for c in range(COMPS):
            q1, x1, q2, x2 = CURL[c]
            for a in range(3):
                m1 = block[METRIC + 3 * a + x1 : METRIC + 3 * a + x1 + 1, :]
                m2 = block[METRIC + 3 * a + x2 : METRIC + 3 * a + x2 + 1, :]
                stack[a * DP : a * DP + NPM, :] = m1 * coefs[q1] - m2 * coefs[q2]
            stack[3 * DP : BIG, :] = flux[c]
            result = dot3(big, split(stack[...]), ((1,), (0,)))
            out_ref[c * NPM : (c + 1) * NPM, g * cap : (g + 1) * cap] = result[:NPM]


def local(groups, doms, fields, metric, normals, fscale, orders, slots, send_faces, recv_faces, dmat, tmat, lmat):
    own_group = lax.axis_index("grp")
    elements = fields.shape[1]
    cap = elements // 2
    total = groups * cap
    lists = 3 * groups
    list_size = send_faces.shape[0] // lists
    f32 = jnp.float32
    target = ((orders - 1) * cap + slots).reshape(1, elements)
    outgoing = pl.pallas_call(
        functools.partial(bucket_kernel, groups, cap),
        out_shape=jax.ShapeDtypeStruct((groups, ROWS, cap), f32),
        in_specs=[VM] * 5,
        out_specs=VM,
        scratch_shapes=[pltpu.VMEM((ROWS, elements), f32)],
        compiler_params=params(),
        name="bucket",
    )(target, fields, metric, normals, fscale)
    bucket = lax.all_to_all(outgoing, "grp", split_axis=0, concat_axis=0, tiled=True)

    node_total = (own_group + 2) * (own_group + 3) * (own_group + 4) // 6
    mask = (jnp.arange(NPM, dtype=jnp.int32) < node_total).astype(f32)
    deriv = dmat[0].reshape(3, NPM, NPM) * mask[None, :, None] * mask[None, None, :]
    deriv = jnp.pad(jnp.transpose(deriv, (1, 0, 2)), ((0, 0), (0, 0), (0, DP - NPM))).reshape(NPM, 3 * DP)
    lift = jnp.transpose((lmat[0] * mask[:, None]).reshape(NPM, FPTS, FACES), (0, 2, 1))
    lift = jnp.pad(lift, ((0, 0), (0, 0), (0, PP - FPTS))).reshape(NPM, FACES * PP)
    big = jnp.pad(jnp.concatenate([deriv, lift], 1), ((0, DP - NPM), (0, 0)))
    trace = jnp.transpose((tmat[0] * mask[None, :]).reshape(FPTS, FACES, NPM), (1, 0, 2))
    trace = jnp.pad(trace, ((0, 0), (0, PP - FPTS), (0, 0)))
    wide = [
        jnp.pad(trace, ((0, 0), (0, 0), (c * NPM, ROWS - (c + 1) * NPM))) for c in range(COMPS)
    ] + [jnp.zeros((FACES, LANES - TR, ROWS), f32)]
    tt = jnp.concatenate(wide, 1).reshape(FACES * LANES, ROWS)

    outgoing_faces = pl.pallas_call(
        functools.partial(send_kernel, groups, cap, lists, list_size),
        out_shape=jax.ShapeDtypeStruct((lists, TR, list_size), f32),
        in_specs=[SM, VM, VM],
        out_specs=VM,
        scratch_shapes=[pltpu.VMEM((FACES * total + 8, LANES), f32), pltpu.VMEM((2, LANES, LANES), f32)],
        compiler_params=params(),
        name="send",
    )(send_faces, bucket, tt)
    arrived = pl.pallas_call(
        functools.partial(exchange_kernel, groups, doms),
        out_shape=jax.ShapeDtypeStruct((lists, TR, list_size), f32),
        in_specs=[VM],
        out_specs=VM,
        scratch_shapes=[
            pltpu.SemaphoreType.DMA((lists,)),
            pltpu.SemaphoreType.DMA((lists,)),
            pltpu.SemaphoreType.DMA,
        ],
        compiler_params=params(collective_id=0, has_side_effects=True),
        name="exchange",
    )(outgoing_faces)
    return pl.pallas_call(
        functools.partial(final_kernel, groups, cap, lists, list_size),
        out_shape=jax.ShapeDtypeStruct((GEO, total), f32),
        in_specs=[SM, VM, VM, VM, VM],
        out_specs=VM,
        scratch_shapes=[
            pltpu.VMEM((lists * list_size + 8, LANES), f32),
            pltpu.VMEM((2, LANES, LANES), f32),
            pltpu.VMEM((FACES, TR, cap), f32),
            pltpu.VMEM((COMPS, FACES * PP, cap), f32),
            pltpu.VMEM((BIG, cap), f32),
        ],
        compiler_params=params(),
        name="final",
    )(recv_faces, arrived, bucket, tt, big)


def solution(mesh):
    col = P(None, ("grp", "dom"))
    row = P(("grp", "dom"))
    mat = P("grp", None, None)
    in_specs = (col, col, col, col, row, row, row, row, mat, mat, mat)
    body = functools.partial(local, mesh.shape["grp"], mesh.shape["dom"])
    return jax.shard_map(body, mesh=mesh, in_specs=in_specs, out_specs=col, check_vma=False)
```

```python
import functools

import jax
import jax.numpy as jnp
from jax import lax
from jax.experimental import pallas as pl
from jax.experimental.pallas import tpu as pltpu
from jax.sharding import PartitionSpec as P

NPM = 35
FPTS = 15
COMPS = 6
FACES = 4
PP = 16
DP = 40
LANES = 128
TR = COMPS * PP
GEO = COMPS * NPM
METRIC, NORMAL, SCALE = GEO, GEO + 9, GEO + 21
ROWS = GEO + 30
BIG = 3 * DP + FACES * PP
MESH = pl.DeviceIdType.MESH
VMEM_LIMIT = 32 * 1024 * 1024


def split(x):
    high = x.astype(jnp.bfloat16)
    low = (x - high.astype(jnp.float32)).astype(jnp.bfloat16)
    return high, low


def dot3(a, b, dims):
    ah, al = a
    bh, bl = b

    def mul(x, y):
        return lax.dot_general(x, y, (dims, ((), ())), preferred_element_type=jnp.float32)

    return mul(ah, bh) + (mul(ah, bl) + mul(al, bh))


def params(**kw):
    return pltpu.CompilerParams(vmem_limit_bytes=VMEM_LIMIT, **kw)


VM = pl.BlockSpec(memory_space=pltpu.VMEM)
SM = pl.BlockSpec(memory_space=pltpu.SMEM)


def partner(g, d, groups):
    if groups & (groups - 1):
        return lax.rem(g + d, groups)
    other = g
    bit = 1
    while bit <= d:
        if d & bit:
            other = other + bit - 2 * bit * lax.rem(g // bit, 2)
        bit *= 2
    return other


def source(g, d, groups):
    if groups & (groups - 1):
        return lax.rem(g - d + groups, groups)
    return partner(g, d, groups)


def bucket_kernel(
    groups, cap, target_ref, fields_ref, metric_ref, normals_ref, fscale_ref, out_ref, pay, sbuf, send_sem, recv_sem
):
    g = lax.axis_index("grp")
    p = lax.axis_index("dom")
    barrier = pltpu.get_barrier_semaphore()
    for d in range(1, groups):
        pl.semaphore_signal(barrier, inc=1, device_id=(partner(g, d, groups), p), device_id_type=MESH)
    pay[0:GEO, :] = fields_ref[...]
    pay[METRIC : METRIC + 9, :] = metric_ref[...]
    pay[NORMAL : NORMAL + 12, :] = normals_ref[...]
    pay[SCALE : SCALE + 4, :] = fscale_ref[...]
    pay[SCALE + 4 : ROWS, :] = jnp.zeros((ROWS - SCALE - 4, pay.shape[1]), jnp.float32)
    high, low = split(pay[...])
    elements = pay.shape[1]
    target = target_ref[...]
    step = min(cap, 256)
    dims = (((1,), (1,)), ((), ()))

    def build(h, dst):
        for k in range(0, cap, step):
            ids = lax.broadcasted_iota(jnp.int32, (step, elements), 0) + (h * cap + k)
            hot = jnp.where(ids == target, 1.0, 0.0).astype(jnp.bfloat16)
            dst[:, k : k + step] = lax.dot_general(
                high, hot, dims, preferred_element_type=jnp.float32
            ) + lax.dot_general(low, hot, dims, preferred_element_type=jnp.float32)

    copies = [
        pltpu.make_async_remote_copy(
            src_ref=sbuf.at[d - 1],
            dst_ref=out_ref.at[g],
            send_sem=send_sem.at[d - 1],
            recv_sem=recv_sem.at[d - 1],
            device_id=(partner(g, d, groups), p),
            device_id_type=MESH,
        )
        for d in range(1, groups)
    ]
    build(partner(g, 1, groups), sbuf.at[0])
    pl.semaphore_wait(barrier, groups - 1)
    for d in range(2, groups):
        build(partner(g, d, groups), sbuf.at[d - 1])
        copies[d - 2].start()
    build(g, out_ref.at[g])
    copies[groups - 2].start()
    for d in range(1, groups):
        src = source(g, d, groups)
        pltpu.make_async_remote_copy(
            src_ref=sbuf.at[d - 1],
            dst_ref=out_ref.at[src],
            send_sem=send_sem.at[d - 1],
            recv_sem=recv_sem.at[d - 1],
            device_id=(partner(g, d, groups), p),
            device_id_type=MESH,
        ).wait_recv()
    for copy in copies:
        copy.wait_send()


def gather_block(index_ref, base, table, tmp):
    for i in range(LANES):
        tmp[i : i + 1, :] = table[pl.ds(index_ref[base + i], 1), :]


def exchange_kernel(
    groups, doms, cap, list_size, send_ref, bucket_ref, tt_ref, out_ref, table, tmp, sbuf, arrived, send_sem, recv_sem
):
    g = lax.axis_index("grp")
    p = lax.axis_index("dom")
    slots = groups * cap
    blocks = list_size // LANES
    lists = 3 * groups
    plan = [(d, j) for j in (2, 0, 1) for d in (1, 2, 0) if (d, j) != (0, 1) and d < groups]
    plan += [(d, j) for d in range(3, groups) for j in (2, 0, 1)]
    barrier = pltpu.get_barrier_semaphore()

    def peer(d, j):
        return (partner(g, d, groups), lax.rem(p + j - 1 + doms, doms))

    for d, j in plan:
        pl.semaphore_signal(barrier, inc=1, device_id=peer(d, j), device_id_type=MESH)

    weights = split(tt_ref[...])
    for b in range(groups):
        coefs = split(bucket_ref[b])
        for f in range(FACES):
            w = tuple(x[f * LANES : (f + 1) * LANES, :] for x in weights)
            table[f * slots + b * cap : f * slots + (b + 1) * cap, :] = dot3(coefs, w, ((0,), (1,)))
    table[FACES * slots : FACES * slots + 8, :] = jnp.zeros((8, LANES), jnp.float32)
    pl.semaphore_wait(barrier, len(plan))

    copies = []
    for n, (d, j) in enumerate(plan):
        base = (j * groups + partner(g, d, groups)) * list_size

        def pair(i, _, n=n, base=base):
            for k in range(2):
                at = pl.multiple_of((2 * i + k) * LANES, LANES)
                gather_block(send_ref, base + at, table, tmp.at[k])
                sbuf[n, :, pl.ds(at, LANES)] = tmp[k].T[:TR]
            return 0

        lax.fori_loop(0, blocks // 2, pair, 0)
        copies.append(
            pltpu.make_async_remote_copy(
                src_ref=sbuf.at[n],
                dst_ref=arrived.at[n],
                send_sem=send_sem.at[n],
                recv_sem=recv_sem.at[n],
                device_id=peer(d, j),
                device_id_type=MESH,
            )
        )
        if n:
            copies[n - 1].start()

    own = (groups + g) * list_size

    def own_block(i, _):
        at = pl.multiple_of(own + i * LANES, LANES)
        gather_block(send_ref, at, table, tmp.at[0])
        out_ref[pl.ds(at, LANES), :] = tmp[0]
        return 0

    lax.fori_loop(0, blocks, own_block, 0)
    copies[-1].start()
    out_ref[lists * list_size : lists * list_size + 8, :] = jnp.zeros((8, LANES), jnp.float32)
    fill = jnp.zeros((LANES - TR, LANES), jnp.float32)
    for n, (d, j) in enumerate(plan):
        copies[n].wait_recv()
        base = (j * groups + source(g, d, groups)) * list_size
        for q in range(blocks):
            block = jnp.concatenate([arrived[n, :, q * LANES : (q + 1) * LANES], fill], 0)
            out_ref[pl.ds(pl.multiple_of(base + q * LANES, LANES), LANES), :] = block.T
    for copy in copies:
        copy.wait_send()


def cross_of(u, v):
    return [u[1] * v[2] - u[2] * v[1], u[2] * v[0] - u[0] * v[2], u[0] * v[1] - u[1] * v[0]]


CURL = ((5, 1, 4, 2), (3, 2, 5, 0), (4, 0, 3, 1), (1, 2, 2, 1), (2, 0, 0, 2), (0, 1, 1, 0))


def final_kernel(
    groups, cap, recv_ref, table, bucket_ref, tt_ref, big_ref, out_ref, tmp, far, flux, stack
):
    slots = groups * cap
    stack[...] = jnp.zeros_like(stack)
    weights = split(tt_ref[...])
    big = split(big_ref[...])

    for g in range(groups):

        def one_face(f, _):
            for q in range(cap // LANES):
                gather_block(recv_ref, f * slots + g * cap + q * LANES, table, tmp.at[q % 2])
                far[f, :, q * LANES : (q + 1) * LANES] = tmp[q % 2].T[:TR]
            return 0

        lax.fori_loop(0, FACES, one_face, 0)
        block = bucket_ref[g]
        pieces = split(block)
        for f in range(FACES):
            own = dot3(tuple(x[f * LANES : f * LANES + TR, :] for x in weights), pieces, ((1,), (0,)))
            jump = far[f] - own
            jumps = [jump[c * PP : (c + 1) * PP, :] for c in range(COMPS)]
            n = [block[NORMAL + c * FACES + f : NORMAL + c * FACES + f + 1, :] for c in range(3)]
            s = 0.5 * block[SCALE + f : SCALE + f + 1, :]
            je, jh = jumps[:3], jumps[3:]
            ne = n[0] * je[0] + n[1] * je[1] + n[2] * je[2]
            nh = n[0] * jh[0] + n[1] * jh[1] + n[2] * jh[2]
            th, te = cross_of(n, jh), cross_of(n, je)
            for c in range(3):
                flux[c, f * PP : (f + 1) * PP, :] = s * (th[c] + je[c] - n[c] * ne)
                flux[3 + c, f * PP : (f + 1) * PP, :] = s * (jh[c] - te[c] - n[c] * nh)
        coefs = [bucket_ref[g, c * NPM : (c + 1) * NPM, :] for c in range(COMPS)]
        for c in range(COMPS):
            q1, x1, q2, x2 = CURL[c]
            for a in range(3):
                m1 = block[METRIC + 3 * a + x1 : METRIC + 3 * a + x1 + 1, :]
                m2 = block[METRIC + 3 * a + x2 : METRIC + 3 * a + x2 + 1, :]
                stack[a * DP : a * DP + NPM, :] = m1 * coefs[q1] - m2 * coefs[q2]
            stack[3 * DP : BIG, :] = flux[c]
            result = dot3(big, split(stack[...]), ((1,), (0,)))
            out_ref[c * NPM : (c + 1) * NPM, g * cap : (g + 1) * cap] = result[:NPM]


def local(groups, doms, fields, metric, normals, fscale, orders, slots, send_faces, recv_faces, dmat, tmat, lmat):
    own_group = lax.axis_index("grp")
    elements = fields.shape[1]
    cap = elements // 2
    total = groups * cap
    lists = 3 * groups
    list_size = send_faces.shape[0] // lists
    f32 = jnp.float32
    target = ((orders - 1) * cap + slots).reshape(1, elements)
    bucket = pl.pallas_call(
        functools.partial(bucket_kernel, groups, cap),
        out_shape=jax.ShapeDtypeStruct((groups, ROWS, cap), f32),
        in_specs=[VM] * 5,
        out_specs=VM,
        scratch_shapes=[
            pltpu.VMEM((ROWS, elements), f32),
            pltpu.VMEM((groups - 1, ROWS, cap), f32),
            pltpu.SemaphoreType.DMA((groups - 1,)),
            pltpu.SemaphoreType.DMA((groups - 1,)),
        ],
        compiler_params=params(collective_id=1, has_side_effects=True),
        name="bucket",
    )(target, fields, metric, normals, fscale)

    node_total = (own_group + 2) * (own_group + 3) * (own_group + 4) // 6
    mask = (jnp.arange(NPM, dtype=jnp.int32) < node_total).astype(f32)
    deriv = dmat[0].reshape(3, NPM, NPM) * mask[None, :, None] * mask[None, None, :]
    deriv = jnp.pad(jnp.transpose(deriv, (1, 0, 2)), ((0, 0), (0, 0), (0, DP - NPM))).reshape(NPM, 3 * DP)
    lift = jnp.transpose((lmat[0] * mask[:, None]).reshape(NPM, FPTS, FACES), (0, 2, 1))
    lift = jnp.pad(lift, ((0, 0), (0, 0), (0, PP - FPTS))).reshape(NPM, FACES * PP)
    big = jnp.pad(jnp.concatenate([deriv, lift], 1), ((0, DP - NPM), (0, 0)))
    trace = jnp.transpose((tmat[0] * mask[None, :]).reshape(FPTS, FACES, NPM), (1, 0, 2))
    trace = jnp.pad(trace, ((0, 0), (0, PP - FPTS), (0, 0)))
    wide = [
        jnp.pad(trace, ((0, 0), (0, 0), (c * NPM, ROWS - (c + 1) * NPM))) for c in range(COMPS)
    ] + [jnp.zeros((FACES, LANES - TR, ROWS), f32)]
    tt = jnp.concatenate(wide, 1).reshape(FACES * LANES, ROWS)

    received = pl.pallas_call(
        functools.partial(exchange_kernel, groups, doms, cap, list_size),
        out_shape=jax.ShapeDtypeStruct((lists * list_size + 8, LANES), f32),
        in_specs=[SM, VM, VM],
        out_specs=VM,
        scratch_shapes=[
            pltpu.VMEM((FACES * total + 8, LANES), f32),
            pltpu.VMEM((2, LANES, LANES), f32),
            pltpu.VMEM((lists - 1, TR, list_size), f32),
            pltpu.VMEM((lists - 1, TR, list_size), f32),
            pltpu.SemaphoreType.DMA((lists - 1,)),
            pltpu.SemaphoreType.DMA((lists - 1,)),
        ],
        compiler_params=params(collective_id=0, has_side_effects=True),
        name="exchange",
    )(send_faces, bucket, tt)
    return pl.pallas_call(
        functools.partial(final_kernel, groups, cap),
        out_shape=jax.ShapeDtypeStruct((GEO, total), f32),
        in_specs=[SM, VM, VM, VM, VM],
        out_specs=VM,
        scratch_shapes=[
            pltpu.VMEM((2, LANES, LANES), f32),
            pltpu.VMEM((FACES, TR, cap), f32),
            pltpu.VMEM((COMPS, FACES * PP, cap), f32),
            pltpu.VMEM((BIG, cap), f32),
        ],
        compiler_params=params(),
        name="final",
    )(recv_faces, received, bucket, tt, big)


def solution(mesh):
    col = P(None, ("grp", "dom"))
    row = P(("grp", "dom"))
    mat = P("grp", None, None)
    in_specs = (col, col, col, col, row, row, row, row, mat, mat, mat)
    body = functools.partial(local, mesh.shape["grp"], mesh.shape["dom"])
    return jax.shard_map(body, mesh=mesh, in_specs=in_specs, out_specs=col, check_vma=False)
```
